1024 devices in a mesh: head: 8 (over x, z_hi), outer: 4 (over y), inner: 32 (over z_lo, core).
Axes of the slice: x: 4, y: 4, z: 32 (z_hi: 2, z_lo: 16; z = z_hi * 16 + z_lo), core: 2. Of those that a mesh axis runs over, the one named last changes fastest.
Arguments:
- queries: bfloat16 [128, 256, 4096], P(('outer', 'inner'), 'head'), may hold values from -120 to 120
- keys: bfloat16 [128, 256, 1024], P(('outer', 'inner'), 'head'), may hold values from -6 to 6
- values: bfloat16 [128, 256, 1024], P(('outer', 'inner'), 'head'), may hold values from -6 to 6
- doc_lengths: int32 [16], replicated, may hold values from 1 to 4096, 32768 in all
Outputs:
- attended: bfloat16 [128, 256, 4096], P(('outer', 'inner'), 'head')
The draws below stay inside these ranges and needn't reach their ends.
Inputs may be any that keep to these rules, and one draw needn't show every extreme that they name: `doc_lengths`: the documents of the packed sequence in order, summing to 32768.
All inputs are finite; a program needn't handle non-finite values.
Results may differ from the reference program's by a relative error of at most 0.0044.
Values may be sent and summed in bfloat16 or wider, within the bound.
No kernel may reach another device: no remote copies, remote signals or barrier semaphores. Data moves between devices by JAX's collectives and lax.ppermute only.
A program may use at most 32 MiB of HBM per device.

```python
import math
import jax
import jax.numpy as jnp
import numpy as np
from jax import lax

HD = 128
QH = 32
KVH = 8
GROUP = 4
ROWS = 256
CTX = 128
REACH = 16
TOKENS = 32768
DOC_MOST = 4096
NDOCS = 16


def drawn_pair(key):
    base = jax.random.fold_in(key, 4242)
    keys_raw = jax.random.truncated_normal(jax.random.fold_in(base, 1), -6.0, 6.0, (CTX, ROWS, KVH, HD), jnp.float32)
    query_raw = jax.random.truncated_normal(jax.random.fold_in(base, 2), -6.0, 6.0, (CTX, ROWS, KVH, GROUP, HD), jnp.float32)
    return (query_raw, keys_raw)


def draw_queries(key, part):
    query_raw, keys_raw = drawn_pair(key)
    return query_raw.reshape(CTX, ROWS, QH * HD).astype(jnp.bfloat16)


def draw_keys(key, part):
    query_raw, keys_raw = drawn_pair(key)
    return keys_raw.reshape(CTX, ROWS, KVH * HD).astype(jnp.bfloat16)


def steps_of(rng, dims, pieces, low, top_value):
    def one(position, parts):
        steps = jax.random.uniform(jax.random.fold_in(jax.random.fold_in(rng, 6), position), (parts,), jnp.float32, low / len(pieces), top_value / len(pieces))
        return jnp.repeat(jnp.exp(steps), dims[position] // parts).reshape((-1,) + (1,) * (len(dims) - position - 1))

    loudness = one(*pieces[0])
    for cut in pieces[1:]:
        loudness = loudness * one(*cut)
    return loudness


def profile(number_of, total, limit, lean):
    loads = [(1 << 20) // math.isqrt(rank ** lean) + 1 for rank in range(2, number_of + 1)]
    rest, holding = total - limit - (number_of - 1), [1] * (number_of - 1)
    while rest > 0:
        candidates = [i for i in range(number_of - 1) if holding[i] < limit]
        whole, left = sum([loads[i] for i in candidates]), rest
        for i in candidates:
            more = min(limit - holding[i], max(1, left * loads[i] // whole), rest)
            holding[i] = holding[i] + more
            rest = rest - more
    return np.array([limit] + holding)


def ragged(stream_key, amount, total, most, slope):
    if amount == 2:
        one = jax.random.randint(stream_key, (), max(1, total - most), min(most, total - 1) + 1)
        return jnp.stack([one, total - one])
    sizes = jnp.asarray(profile(amount, total, most, slope), jnp.int32)
    twos = (amount - 1) // 2
    source_of, taker = sizes[1:1 + 2 * twos:2], sizes[2:2 + 2 * twos:2]
    slack = jnp.minimum(source_of - 1, most - taker)
    moved = jax.random.randint(jax.random.fold_in(stream_key, 1), (twos,), 0, 1 << 20) % (slack + 1)
    sizes = sizes.at[1:1 + 2 * twos:2].set(source_of - moved).at[2:2 + 2 * twos:2].set(taker + moved)
    return sizes[jax.random.permutation(jax.random.fold_in(stream_key, 2), amount)]


def scatter_about(stream_key, shape, spread, limit, pieces=(), held_as=jnp.bfloat16):
    values = jax.random.normal(stream_key, shape, jnp.float32) * spread
    if len(pieces) > 0:
        values = steps_of(stream_key, shape, pieces, -0.22, 0.18) * values
    return jnp.clip(values, min=-limit, max=limit).astype(held_as)


def setup_inputs(seed: int = 0) -> dict:
    seeds = jax.random.split(jax.random.key(seed), 5)
    queries = draw_queries(jax.random.fold_in(seeds[4], 71), 0)
    keys = draw_keys(jax.random.fold_in(seeds[4], 71), 0)
    values = scatter_about(seeds[2], (CTX, ROWS, KVH * HD), 1.0, 6.0, ((0, 128), (1, 8)))
    doc_lengths = ragged(seeds[3], NDOCS, TOKENS, DOC_MOST, 1).astype(jnp.int32)
    return dict(queries=queries, keys=keys, values=values, doc_lengths=doc_lengths)


def doc_index(positions, doc_lengths):
    ends = jnp.cumsum(doc_lengths)
    return lax.optimization_barrier(jnp.sum((positions[:, None] >= ends[None, :]).astype(jnp.int32), axis=1))

def reference(queries, keys, values, doc_lengths):
    ctx_count = queries.shape[0]
    rows = queries.shape[1]
    margin = REACH * rows
    q_all = queries.reshape(ctx_count * rows, KVH, GROUP, HD)
    k_all = jnp.concatenate([jnp.zeros((margin, KVH, HD), keys.dtype), keys.reshape(ctx_count * rows, KVH, HD)], axis=0)
    v_all = jnp.concatenate([jnp.zeros((margin, KVH, HD), values.dtype), values.reshape(ctx_count * rows, KVH, HD)], axis=0)
    scale = 1.0 / math.sqrt(HD)

    def one_block(rank):
        start = (rank * rows).astype(jnp.int32)
        q_block = lax.dynamic_slice_in_dim(q_all, start, rows, 0).astype(jnp.float32)
        k_block = lax.dynamic_slice_in_dim(k_all, start, margin + rows, 0).astype(jnp.float32)
        v_block = lax.dynamic_slice_in_dim(v_all, start, margin + rows, 0).astype(jnp.float32)
        q_pos = start + jnp.arange(rows, dtype=jnp.int32)
        k_pos = start - margin + jnp.arange(margin + rows, dtype=jnp.int32)
        q_doc = doc_index(q_pos, doc_lengths)
        k_doc = doc_index(k_pos, doc_lengths)
        visible = (k_pos[None, :] >= 0) & (k_pos[None, :] <= q_pos[:, None]) & (k_doc[None, :] == q_doc[:, None])
        scores = jnp.einsum('qgeh,kgh->geqk', q_block, k_block) * scale
        peak = lax.optimization_barrier(jnp.max(jnp.where(visible[None, None], scores, -1e+30), axis=-1))
        weights = jnp.where(visible[None, None], jnp.exp(scores - peak[..., None]), 0.0)
        total = lax.optimization_barrier(jnp.sum(weights, axis=-1))
        rounded = lax.optimization_barrier(weights.astype(jnp.bfloat16)).astype(jnp.float32)
        summed = jnp.einsum('geqk,kgh->qgeh', rounded, v_block)
        result = summed / jnp.transpose(total, (2, 0, 1))[..., None]
        return result.astype(jnp.bfloat16).reshape(rows, KVH * GROUP * HD)
    return lax.map(one_block, jnp.arange(ctx_count, dtype=jnp.int32))
```

```python
import functools
import math

import jax
import jax.numpy as jnp
import numpy as np
from jax import lax
from jax.experimental import pallas as pl
from jax.experimental.pallas import tpu as pltpu
from jax.sharding import Mesh
from jax.sharding import PartitionSpec as P

HD = 128
ROWS = 32
NEG_FILL = -1e30
AXES = ("x", "zh", "y", "zl", "c")
PLANE = ("x", "c")
RING = ("zh", "y", "zl")

STEPS = (
    ("m1", (0,), (-9,), -9),
    ("p1", (0,), (1,), 1),
    ("p2", (1,), (4,), 3),
    ("p3", (4,), (7,), 3),
    ("e1", (1, 4, 7), (2, 5, 8), 1),
    ("f1", (4, 7), (3, 6), -1),
    ("m2", (-9,), (-12,), -3),
    ("m3", (-12,), (-15,), -3),
    ("e2", (-9, -12), (-8, -11), 1),
    ("f2", (-9, -12), (-10, -13), -1),
    ("e3", (-15,), (-14,), 1),
    ("f3", (-15,), (-16,), -1),
)
CALLS = (
    (0, 1, 4, 7),
    (2, 5, 8, 3, 6, -9, -12),
    (-8, -11, -10, -13, -15, -14, -16),
)


class Plan:
    def __init__(self, outer, half, halves):
        length, chips = half * halves, outer * half
        index = lambda z, y: ((z // half) * outer + y) * half + z % half
        where = {(z, y * half + z % half): index(z, y) for z in range(length) for y in range(outer)}
        held = {0: {key: key for key in where}}
        self.pairs = {}
        for name, sent, got, shift in STEPS:
            target = {}
            for slot, new in zip(sent, got):
                held[new] = {}
                for (z, n), (zs, ns) in held[slot].items():
                    z2 = (z + shift) % length
                    to = (z2, (ns + (z2 - zs) % half) % chips)
                    assert target.setdefault((z, n), to) == to
                    held[new][to] = (zs, ns)
            assert len(set(target.values())) == len(target)
            self.pairs[name] = [(where[a], where[b]) for a, b in sorted(target.items())]
        self.slots = [s for call in CALLS for s in call]
        self.codes = np.full((len(where), len(self.slots)), -1, np.int32)
        for j, slot in enumerate(self.slots):
            for (z, n), (zs, ns) in held[slot].items():
                if ns <= n:
                    self.codes[where[z, n], j] = ns * halves + zs // half
        for (z, n), i in where.items():
            want = {m * halves + h for m in range(max(0, n - half // 2), n + 1) for h in range(halves)}
            got = [int(c) for c in self.codes[i] if c >= 0]
            assert len(set(got)) == len(got) and want <= set(got)


def row_offsets(shape, dim):
    i = lax.broadcasted_iota(jnp.int32, shape, dim)
    return ((i // ROWS) % 2) * 256 + (i // (2 * ROWS)) * (2 * ROWS) + i % ROWS


def attend_kernel(slots, first, last, *refs):
    refs = list(refs)
    meta, lengths, q_ref = refs[:3]
    refs = refs[3:]
    kv, refs = refs[: len(slots)], refs[len(slots) :]
    if not first:
        (ml_in, acc_in), refs = refs[:2], refs[2:]
    if last:
        out_ref, ml, acc = refs
    else:
        ml, acc = refs
    unit = math.log2(math.e) / math.sqrt(HD)

    me = meta[0]
    base = (me // 2) * 512 + (me % 2) * ROWS
    low, high = base, base + 256 + 6 * ROWS + ROWS - 1

    def start_of(pos):
        def step(d, carry):
            end, begin = carry
            end = end + lengths[d]
            return end, jnp.where(end <= pos, end, begin)

        return lax.fori_loop(0, lengths.shape[0], step, (jnp.int32(0), pos * 0))[1]

    low_start, high_start = start_of(low), start_of(high)
    q_pos = base + row_offsets((256, 1), 0)
    q_start = start_of(q_pos)

    if not first:
        ml[...] = ml_in[...]
        acc[...] = acc_in[...]

    def fold(block, masked, fresh, k_base):
        k = block[:, 0].reshape(256, HD)
        v = block[:, 1].reshape(256, HD)
        if masked:
            k_pos = k_base + row_offsets((1, 256), 1)
            bias = jnp.where((k_pos <= q_pos) & (k_pos >= q_start), 0.0, NEG_FILL)
        for h in range(4):
            cols = slice(h * HD, (h + 1) * HD)
            s = lax.dot_general(
                q_ref[:, cols], k, (((1,), (1,)), ((), ())), preferred_element_type=jnp.float32
            )
            if masked:
                s = s + bias
            top = jnp.max(s, axis=1, keepdims=True)
            if not fresh:
                before = ml[:, h : h + 1]
                top = jnp.maximum(before, top)
                factor = jnp.exp2((before - top) * unit)
            w = jnp.exp2((s - top) * unit)
            total = jnp.sum(w, axis=1, keepdims=True)
            added = jnp.dot(w.astype(jnp.bfloat16), v, preferred_element_type=jnp.float32)
            if not fresh:
                total = total + ml[:, 4 + h : 5 + h] * factor
                added = added + acc[:, cols] * factor
            ml[:, h : h + 1] = top
            ml[:, 4 + h : 5 + h] = total
            acc[:, cols] = added

    for j, (ref, i) in enumerate(zip(kv, slots)):
        code = meta[1 + j]
        k_base = (code // 2) * 512 + (code % 2) * ROWS
        k_high = k_base + 256 + 6 * ROWS + ROWS - 1
        if first and j == 0:
            fold(ref[i], True, True, k_base)
            continue
        seen = (code >= 0) & (k_high >= low_start) & (k_base <= high)
        whole = (k_base >= high_start) & (k_high <= low)

        @pl.when(seen & whole)
        def _(ref=ref, i=i, k_base=k_base):
            fold(ref[i], False, False, k_base)

        @pl.when(seen & jnp.logical_not(whole))
        def _(ref=ref, i=i, k_base=k_base):
            fold(ref[i], True, False, k_base)

    if last:
        for h in range(4):
            cols = slice(h * HD, (h + 1) * HD)
            res = (acc[:, cols] / ml[:, 4 + h : 5 + h]).astype(jnp.bfloat16)
            out_ref[:, :, cols] = res.reshape(8, ROWS, HD)


def attend(meta, lengths, q, blocks, state, last, name):
    n = len(blocks)
    vmem = pl.BlockSpec(memory_space=pltpu.VMEM)
    smem = pl.BlockSpec(memory_space=pltpu.SMEM)
    first = state is None
    ml = jax.ShapeDtypeStruct((256, 8), jnp.float32)
    acc = jax.ShapeDtypeStruct((256, 4 * HD), jnp.float32)
    out = jax.ShapeDtypeStruct((8, ROWS, 4 * HD), jnp.bfloat16)
    return pl.pallas_call(
        functools.partial(attend_kernel, tuple(i for _, i in blocks), first, last),
        out_shape=out if last else (ml, acc),
        in_specs=[smem, smem, vmem] + [vmem] * n + ([] if first else [vmem] * 2),
        out_specs=vmem if last else (vmem, vmem),
        scratch_shapes=[pltpu.VMEM(ml.shape, ml.dtype), pltpu.VMEM(acc.shape, acc.dtype)]
        if last
        else [],
        name=name,
        cost_estimate=pl.CostEstimate(
            flops=n * 4 * 256 * 256 * HD * 4,
            bytes_accessed=n * 131072 + 1500000,
            transcendentals=n * 4 * 256 * 256,
        ),
    )(meta, lengths, q, *[b for b, _ in blocks], *(() if first else state))


def body(plan, queries, keys, values, doc_lengths):
    kv = jnp.stack([keys[0].reshape(ROWS, 8, HD), values[0].reshape(ROWS, 8, HD)], axis=1)
    kv = jnp.transpose(kv, (2, 1, 0, 3))
    with jax.named_scope("kv_swap"):
        own = lax.all_to_all(kv, PLANE, split_axis=0, concat_axis=0, tiled=True)
    q = jnp.transpose(queries[0].reshape(ROWS, 8, 4 * HD), (1, 0, 2))
    with jax.named_scope("q_swap"):
        q = lax.all_to_all(q, PLANE, split_axis=0, concat_axis=0, tiled=True)
    q = q.reshape(8 * ROWS, 4 * HD)

    place = lax.axis_index(RING)
    me = (lax.axis_index("y") * 16 + lax.axis_index("zl")) * 2 + lax.axis_index("zh")
    codes = lax.dynamic_index_in_dim(jnp.asarray(plan.codes), place, 0, keepdims=False)

    held = {0: (own[None], 0)}
    for name, sent, got, _ in STEPS:
        parts = [held[s][0][held[s][1]] for s in sent]
        with jax.named_scope(name):
            back = lax.ppermute(jnp.stack(parts), RING, plan.pairs[name])
        for i, s in enumerate(got):
            held[s] = (back, i)

    state, at = None, 0
    for j, call in enumerate(CALLS):
        meta = jnp.concatenate([me[None], codes[at : at + len(call)]])
        at += len(call)
        with jax.named_scope(f"attend{j}"):
            state = attend(
                meta,
                doc_lengths,
                q,
                [held[s] for s in call],
                state,
                j == len(CALLS) - 1,
                f"attend{j}",
            )
    with jax.named_scope("o_swap"):
        out = lax.all_to_all(state, PLANE, split_axis=0, concat_axis=0, tiled=True)
    return jnp.transpose(out, (1, 0, 2)).reshape(1, ROWS, 32 * HD)


def solution(mesh):
    fine = Mesh(mesh.devices.reshape(4, 2, 4, 16, 2), AXES)
    spec = P(("y", "zl", "c"), ("x", "zh"), None)
    return jax.shard_map(
        functools.partial(body, Plan(4, 16, 2)),
        mesh=fine,
        in_specs=(spec, spec, spec, P()),
        out_specs=spec,
        check_vma=False,
    )
```

```python
import functools
import math

import jax
import jax.numpy as jnp
from jax import lax
from jax.experimental import pallas as pl
from jax.experimental.pallas import tpu as pltpu
from jax.sharding import Mesh
from jax.sharding import PartitionSpec as P


HD = 128
ROWS = 32
HEADS = 4
CHUNK = 64
NEG_FILL = -1e30
AXES = ("x", "zh", "y", "zl", "c")
PLANE = ("x", "c")
RING = ("zh", "y", "zl")

STEPS = (
    ("m1", (0,), (-9,), -9),
    ("p1", (0,), (3,), 3),
    ("p2", (3,), (6,), 3),
    ("m2", (-9,), (-12,), -3),
    ("e1", (0, 3, 6), (1, 4, 7), 1),
    ("m3", (-12,), (-15,), -3),
    ("g1", (-9, -12, 3, 6), (-10, -13, 2, 5), -1),
    ("g2", (-9, -12, 7), (-8, -11, 8), 1),
    ("h1", (-15,), (-16,), -1),
    ("h2", (-15,), (-14,), 1),
)
CALLS = (
    (0, 3, 6),
    (1, 4, 7, -9, -12),
    (2, 5, 8, -10, -13, -8, -11, -15),
    (-16, -14),
)


class Plan:
    def __init__(self, outer, half, halves):
        length, chips = half * halves, outer * half
        index = lambda z, y: ((z // half) * outer + y) * half + z % half
        where = {(z, y * half + z % half): index(z, y) for z in range(length) for y in range(outer)}
        held = {0: {key: key for key in where}}
        self.pairs = {}
        for name, sent, got, shift in STEPS:
            target = {}
            for slot, new in zip(sent, got):
                held[new] = {}
                for (z, n), (zs, ns) in held[slot].items():
                    z2 = (z + shift) % length
                    to = (z2, (ns + (z2 - zs) % half) % chips)
                    assert target.setdefault((z, n), to) == to
                    held[new][to] = (zs, ns)
            assert len(set(target.values())) == len(target)
            self.pairs[name] = [(where[a], where[b]) for a, b in sorted(target.items())]
        for (z, n) in where:
            want = {(h * half + m % half, m) for m in range(max(0, n - half // 2), n + 1) for h in range(halves)}
            got = [held[s][z, n] for call in CALLS for s in call]
            assert len(set(got)) == len(got) and want <= set(got)


def row_offsets(shape, dim):
    i = lax.broadcasted_iota(jnp.int32, shape, dim)
    return ((i >> 5) & 1) * 256 + (i >> 6) * 64 + (i & 31)


def attend_kernel(slots, first, last, *refs):
    count = len(slots)
    refs = list(refs)
    lengths, q_ref = refs[:2]
    refs = refs[2:]
    arrays = max(a for _, a, _ in slots) + 1
    kv, refs = refs[:arrays], refs[arrays:]
    if not first:
        (start_ref, top_in, acc_in), refs = refs[:3], refs[3:]
    if last:
        out_ref, *scores, k_all, v_all, bias, tops = refs
    elif first:
        start_ref, tops, acc_out, *scores, k_all, v_all, bias = refs
    else:
        tops, acc_out, *scores, k_all, v_all, bias = refs
    scores, rounded = scores[:2], scores[2:]
    unit = math.log2(math.e) / math.sqrt(HD)
    half, halves = lax.axis_size("zl"), lax.axis_size("zh")

    chip = lax.axis_index("y") * half + lax.axis_index("zl")
    zh = lax.axis_index("zh")
    low = chip * 512 + zh * ROWS
    reach = 256 + 6 * ROWS + ROWS - 1

    def start_of(pos):
        end, begin = jnp.int32(0), pos * 0
        for d in range(lengths.shape[0]):
            end = end + lengths[d]
            begin = jnp.where(end <= pos, end, begin)
        return begin

    high_start = start_of(low + reach)
    q_pos = low + row_offsets((256, 1), 0)
    if first:
        start_ref[...] = start_of(q_pos)
    partial = []
    for j, (slot, a, i) in enumerate(slots):
        back = slot if slot >= 0 else slot + half
        from_zh = ((zh * half + lax.axis_index("zl") - slot + half * halves) >> 4) & 1
        k_base = (chip - back) * 512 + from_zh * ROWS
        partial.append((k_base < high_start) | (k_base + reach > low))

        @pl.when(partial[j])
        def _(j=j, k_base=k_base):
            k_pos = k_base + row_offsets((1, 256), 1)
            seen = (k_pos <= q_pos) & (k_pos >= start_ref[...])
            bias[:, j * 256 : (j + 1) * 256] = jnp.where(seen, 0.0, NEG_FILL)

        k_all[j * 256 : (j + 1) * 256] = kv[a][i, :, 0].reshape(256, HD)
        v_all[j * 256 : (j + 1) * 256, :HD] = kv[a][i, :, 1].reshape(256, HD)

    v_all[:, HD:] = jnp.ones((count * 256, HD), jnp.bfloat16)

    def score(h):
        q = q_ref[:, h].reshape(256, HD)
        scores[h & 1][...] = lax.dot_general(
            q, k_all[...], (((1,), (1,)), ((), ())), preferred_element_type=jnp.float32
        )

    def hide(h):
        for j in range(count):

            @pl.when(partial[j])
            def _(j=j):
                cols = slice(j * 256, (j + 1) * 256)
                scores[h & 1][:, cols] = scores[h & 1][:, cols] + bias[:, cols]

    def weigh(h):
        for r in range(0, 256, CHUNK):
            rows = slice(r, r + CHUNK)
            wide = scores[h & 1][rows, :256]
            for j in range(1, count):
                wide = jnp.maximum(wide, scores[h & 1][rows, j * 256 : (j + 1) * 256])
            top = jnp.max(wide, axis=1, keepdims=True)
            if not first:
                top = jnp.maximum(top_in[h, rows], top)
            for j in range(count):
                cols = slice(j * 256, (j + 1) * 256)
                w = jnp.exp2((scores[h & 1][rows, cols] - top) * unit)
                rounded[h & 1][rows, cols] = w.astype(jnp.bfloat16)
            tops[h, rows] = top

    def gather(h):
        for r in range(0, 256, 128):
            rows = slice(r, r + 128)
            added = jnp.dot(rounded[h & 1][rows], v_all[...], preferred_element_type=jnp.float32)
            if not first:
                factor = jnp.exp2((top_in[h, rows] - tops[h, rows]) * unit)
                added = added + acc_in[h, rows] * factor
            if last:
                res = added[:, :HD] / added[:, HD:]
                out_ref[r // ROWS : r // ROWS + 4, h] = res.astype(jnp.bfloat16).reshape(4, ROWS, HD)
            else:
                acc_out[h, rows] = added

    for h in range(HEADS + 2):
        if h < HEADS:
            score(h)
        if h >= 2:
            gather(h - 2)
        if 1 <= h <= HEADS:
            weigh(h - 1)
        if h < HEADS:
            hide(h)


VMEM = pl.BlockSpec(memory_space=pltpu.VMEM)
SMEM = pl.BlockSpec(memory_space=pltpu.SMEM)


def attend(lengths, q, slots, blocks, state, last):
    n = len(blocks)
    first = state is None
    start = jax.ShapeDtypeStruct((256, 1), jnp.int32)
    top = jax.ShapeDtypeStruct((HEADS, 256, 1), jnp.float32)
    acc = jax.ShapeDtypeStruct((HEADS, 256, 2 * HD), jnp.float32)
    out = jax.ShapeDtypeStruct((8, HEADS, ROWS, HD), jnp.bfloat16)
    outs = out if last else (start, top, acc) if first else (top, acc)
    arrays = list({id(b): b for b, _ in blocks}.values())
    number = {id(b): a for a, b in enumerate(arrays)}
    where = tuple((s, number[id(b)], i) for s, (b, i) in zip(slots, blocks))
    return pl.pallas_call(
        functools.partial(attend_kernel, where, first, last),
        out_shape=outs,
        in_specs=[SMEM, VMEM] + [VMEM] * len(arrays) + ([] if first else [VMEM] * 3),
        out_specs=VMEM if last else tuple(VMEM for _ in outs),
        scratch_shapes=[
            pltpu.VMEM((256, n * 256), jnp.float32),
            pltpu.VMEM((256, n * 256), jnp.float32),
            pltpu.VMEM((256, n * 256), jnp.bfloat16),
            pltpu.VMEM((256, n * 256), jnp.bfloat16),
            pltpu.VMEM((n * 256, HD), jnp.bfloat16),
            pltpu.VMEM((n * 256, 2 * HD), jnp.bfloat16),
            pltpu.VMEM((256, n * 256), jnp.float32),
        ]
        + ([pltpu.VMEM(top.shape, top.dtype)] if last else []),
        compiler_params=pltpu.CompilerParams(vmem_limit_bytes=(6 + 2 * n) << 20),
        cost_estimate=pl.CostEstimate(
            flops=n * HEADS * 256 * 256 * HD * 4,
            bytes_accessed=n * 131072 + 1500000,
            transcendentals=n * HEADS * 256 * 256,
        ),
    )(lengths, q, *arrays, *(() if first else state))


def pack_kv_kernel(k_ref, v_ref, out_ref):
    for g in range(8):
        out_ref[g, 0] = k_ref[0, :, g * HD : (g + 1) * HD]
        out_ref[g, 1] = v_ref[0, :, g * HD : (g + 1) * HD]


def pack_q_kernel(q_ref, out_ref):
    for g in range(8):
        for h in range(HEADS):
            at = (g * HEADS + h) * HD
            out_ref[g, h] = q_ref[0, :, at : at + HD]


def pack(kernel, shape, *arrays):
    return pl.pallas_call(
        kernel,
        out_shape=jax.ShapeDtypeStruct(shape, jnp.bfloat16),
        in_specs=[VMEM] * len(arrays),
        out_specs=VMEM,
    )(*arrays)


def body(plan, *args):
    return spread(plan, *args)


def spread(plan, queries, keys, values, doc_lengths):
    kv = pack(pack_kv_kernel, (8, 2, ROWS, HD), keys, values)
    own = lax.all_to_all(kv, PLANE, split_axis=0, concat_axis=0, tiled=True)
    q = pack(pack_q_kernel, (8, HEADS, ROWS, HD), queries)
    q = lax.all_to_all(q, PLANE, split_axis=0, concat_axis=0, tiled=True)

    held = {0: (own[None], 0)}
    for name, sent, got, _ in STEPS:
        parts = [held[s][0][held[s][1]] for s in sent]
        back = lax.ppermute(jnp.stack(parts), RING, plan.pairs[name])
        for i, s in enumerate(got):
            held[s] = (back, i)

    state, start = None, None
    for j, call in enumerate(CALLS):
        state = attend(doc_lengths, q, call, [held[s] for s in call], state, j == len(CALLS) - 1)
        if j == 0:
            start, *state = state
        if j < len(CALLS) - 1:
            state = (start, *state)
    out = lax.all_to_all(state, PLANE, split_axis=0, concat_axis=0, tiled=True)
    return jnp.transpose(out, (2, 0, 1, 3)).reshape(1, ROWS, 32 * HD)


def solution(mesh):
    fine = Mesh(mesh.devices.reshape(4, 2, 4, 16, 2), AXES)
    spec = P(("y", "zl", "c"), ("x", "zh"), None)
    return jax.shard_map(
        functools.partial(body, Plan(4, 16, 2)),
        mesh=fine,
        in_specs=(spec, spec, spec, P()),
        out_specs=spec,
        check_vma=False,
    )
```

```python
import functools
import math

import jax
import jax.numpy as jnp
from jax import lax
from jax.experimental import pallas as pl
from jax.experimental.pallas import tpu as pltpu
from jax.sharding import Mesh
from jax.sharding import PartitionSpec as P


HD = 128
ROWS = 32
HEADS = 4
CHUNK = 64
NEG_FILL = -1e30
AXES = ("x", "zh", "y", "zl", "c")
PLANE = ("x", "c")
RING = ("zh", "y", "zl")

STEPS = (
    ("m1", (0,), (-9,), -9),
    ("p1", (0,), (3,), 3),
    ("p2", (3,), (6,), 3),
    ("m2", (-9,), (-12,), -3),
    ("e1", (0, 3, 6, -9), (1, 4, 7, -8), 1),
    ("m3", (-12,), (-15,), -3),
    ("g2", (1, 4, -12), (2, 5, -11), 1),
    ("g1", (-9, -12), (-10, -13), -1),
    ("h2", (-15, 7), (-14, 8), 1),
    ("h1", (-15,), (-16,), -1),
)
CALLS = (
    (0, 3, 6),
    (1, 4, 7, -8, -9, -12),
    (2, 5, -10, -11, -13, -15),
    (8, -14, -16),
)


class Plan:
    def __init__(self, outer, half, halves):
        length, chips = half * halves, outer * half
        index = lambda z, y: ((z // half) * outer + y) * half + z % half
        where = {(z, y * half + z % half): index(z, y) for z in range(length) for y in range(outer)}
        held = {0: {key: key for key in where}}
        moves = {}
        for name, sent, got, shift in STEPS:
            target = {}
            for slot, new in zip(sent, got):
                held[new] = {}
                for (z, n), (zs, ns) in held[slot].items():
                    z2 = (z + shift) % length
                    to = (z2, (ns + (z2 - zs) % half) % chips)
                    assert target.setdefault((z, n), to) == to
                    held[new][to] = (zs, ns)
            assert len(set(target.values())) == len(target)
            moves[name] = target
        wanted = {s: {key for key in where if at[key][1] <= key[1]} for s, at in held.items()}
        self.pairs = {}
        for name, sent, got, shift in reversed(STEPS):
            used = {a: b for a, b in moves[name].items() if any(b in wanted[s] for s in got)}
            for slot, new in zip(sent, got):
                wanted[slot] |= {a for a, b in used.items() if b in wanted[new]}
            self.pairs[name] = [(where[a], where[b]) for a, b in sorted(used.items())]
        for (z, n) in where:
            want = {(h * half + m % half, m) for m in range(max(0, n - half // 2), n + 1) for h in range(halves)}
            got = [held[s][z, n] for call in CALLS for s in call]
            assert len(set(got)) == len(got) and want <= set(got)


def row_offsets(shape, dim):
    i = lax.broadcasted_iota(jnp.int32, shape, dim)
    return ((i >> 5) & 1) * 256 + (i >> 6) * 64 + (i & 31)


def document_bounds(lengths):
    count = lengths.shape[0]
    lane = lax.broadcasted_iota(jnp.int32, (1, HD), 1)
    begin = jnp.where(lane == count, -(1 << 24), 1 << 24)
    end = jnp.where(lane == count, 0, -(1 << 24))
    at = jnp.int32(0)
    for d in range(count):
        begin = jnp.where(lane == d, at, begin)
        at = at + lengths[d]
        end = jnp.where(lane == d, at, end)
    return begin, end


def attend_kernel(slots, first, last, *refs):
    count = len(slots)
    refs = list(refs)
    arrays = max(a for _, a, _ in slots) + 1
    if first:
        lengths, q_ref, *refs = refs
    else:
        bounds, q_all, top_in, acc_in, *refs = refs
    kv, refs = refs[:arrays], refs[arrays:]
    if last:
        out_ref, tops, *refs = refs
    elif first:
        bounds, q_all, tops, acc_out, *refs = refs
    else:
        tops, acc_out, *refs = refs
    k_all, v_all, *refs = refs
    scores, rounded = refs[:2], refs[2:]
    unit = math.log2(math.e) / math.sqrt(HD)
    half, halves = lax.axis_size("zl"), lax.axis_size("zh")

    chip = lax.axis_index("y") * half + lax.axis_index("zl")
    zh = lax.axis_index("zh")
    offsets = row_offsets((256, HD), 0)

    def members(base):
        return (offsets >= bounds[0:1] - base) & (offsets < bounds[1:2] - base)

    if first:
        begin, end = document_bounds(lengths)
        bounds[0:1], bounds[1:2] = begin, end
        apart = jnp.where(members(chip * 512 + zh * ROWS), 0.0, NEG_FILL).astype(jnp.bfloat16)
        for h in range(HEADS):
            q_all[h, :, :HD] = q_ref[:, h].reshape(256, HD)
            q_all[h, :, HD:] = apart

    later = {}
    for j, (slot, a, i) in enumerate(slots):
        rows = slice(j * 256, (j + 1) * 256)
        back = slot if slot >= 0 else slot + half
        from_zh = ((zh * half + lax.axis_index("zl") - slot + half * halves) >> 4) & 1
        base = (chip - back) * 512 + from_zh * ROWS
        k_all[rows, :HD] = kv[a][i, :, 0].reshape(256, HD)
        k_all[rows, HD:] = jnp.where(members(base), 1.0, 0.0).astype(jnp.bfloat16)
        v_all[rows, :HD] = kv[a][i, :, 1].reshape(256, HD)
        if back == 0:
            later[j] = (from_zh - zh) * ROWS
    v_all[:, HD:] = jnp.ones((count * 256, HD), jnp.bfloat16)

    def score(h):
        scores[h & 1][...] = lax.dot_general(
            q_all[h], k_all[...], (((1,), (1,)), ((), ())), preferred_element_type=jnp.float32
        )

    def weigh(h):
        for r in range(0, 256, CHUNK):
            rows = slice(r, r + CHUNK)
            wide = None
            for j in range(count):
                cols = slice(j * 256, (j + 1) * 256)
                s = scores[h & 1][rows, cols]
                if j in later:
                    q_at = row_offsets((256, 1), 0)[rows] - later[j]
                    s = jnp.where(row_offsets((1, 256), 1) <= q_at, s, NEG_FILL)
                    scores[h & 1][rows, cols] = s
                wide = s if wide is None else jnp.maximum(wide, s)
            top = jnp.max(wide, axis=1, keepdims=True)
            if not first:
                top = jnp.maximum(top_in[h, rows], top)
            for j in range(count):
                cols = slice(j * 256, (j + 1) * 256)
                w = jnp.exp2((scores[h & 1][rows, cols] - top) * unit)
                rounded[h & 1][rows, cols] = w.astype(jnp.bfloat16)
            tops[h, rows] = top

    def gather(h):
        for r in range(0, 256, 128):
            rows = slice(r, r + 128)
            added = jnp.dot(rounded[h & 1][rows], v_all[...], preferred_element_type=jnp.float32)
            if not first:
                factor = jnp.exp2((top_in[h, rows] - tops[h, rows]) * unit)
                added = added + acc_in[h, rows] * factor
            if last:
                res = added[:, :HD] / added[:, HD:]
                out_ref[r // ROWS : r // ROWS + 4, h] = res.astype(jnp.bfloat16).reshape(4, ROWS, HD)
            else:
                acc_out[h, rows] = added

    for h in range(HEADS + 2):
        if h < HEADS:
            score(h)
        if h >= 2:
            gather(h - 2)
        if 1 <= h <= HEADS:
            weigh(h - 1)


VMEM = pl.BlockSpec(memory_space=pltpu.VMEM)
SMEM = pl.BlockSpec(memory_space=pltpu.SMEM)


def attend(heads_in, slots, blocks, state, last):
    n = len(blocks)
    first = state is None
    bounds = jax.ShapeDtypeStruct((8, HD), jnp.int32)
    q_all = jax.ShapeDtypeStruct((HEADS, 256, 2 * HD), jnp.bfloat16)
    top = jax.ShapeDtypeStruct((HEADS, 256, 1), jnp.float32)
    acc = jax.ShapeDtypeStruct((HEADS, 256, 2 * HD), jnp.float32)
    out = jax.ShapeDtypeStruct((8, HEADS, ROWS, HD), jnp.bfloat16)
    outs = out if last else (bounds, q_all, top, acc) if first else (top, acc)
    arrays = list({id(b): b for b, _ in blocks}.values())
    number = {id(b): a for a, b in enumerate(arrays)}
    where = tuple((s, number[id(b)], i) for s, (b, i) in zip(slots, blocks))
    return pl.pallas_call(
        functools.partial(attend_kernel, where, first, last),
        out_shape=outs,
        in_specs=([SMEM, VMEM] if first else [VMEM] * 4) + [VMEM] * len(arrays),
        out_specs=VMEM if last else tuple(VMEM for _ in outs),
        scratch_shapes=([pltpu.VMEM(top.shape, top.dtype)] if last else [])
        + [
            pltpu.VMEM((n * 256, 2 * HD), jnp.bfloat16),
            pltpu.VMEM((n * 256, 2 * HD), jnp.bfloat16),
            pltpu.VMEM((256, n * 256), jnp.float32),
            pltpu.VMEM((256, n * 256), jnp.float32),
            pltpu.VMEM((256, n * 256), jnp.bfloat16),
            pltpu.VMEM((256, n * 256), jnp.bfloat16),
        ],
        compiler_params=pltpu.CompilerParams(vmem_limit_bytes=(6 + 2 * n) << 20),
        cost_estimate=pl.CostEstimate(
            flops=n * HEADS * 256 * 256 * HD * 4,
            bytes_accessed=n * 131072 + 1500000,
            transcendentals=n * HEADS * 256 * 256,
        ),
    )(*heads_in, *(() if first else state), *arrays)


def pack_kv_kernel(k_ref, v_ref, out_ref):
    for g in range(8):
        out_ref[g, 0] = k_ref[0, :, g * HD : (g + 1) * HD]
        out_ref[g, 1] = v_ref[0, :, g * HD : (g + 1) * HD]


def pack_q_kernel(q_ref, out_ref):
    for g in range(8):
        for h in range(HEADS):
            at = (g * HEADS + h) * HD
            out_ref[g, h] = q_ref[0, :, at : at + HD]


def pack(kernel, shape, *arrays):
    return pl.pallas_call(
        kernel,
        out_shape=jax.ShapeDtypeStruct(shape, jnp.bfloat16),
        in_specs=[VMEM] * len(arrays),
        out_specs=VMEM,
    )(*arrays)


def body(plan, *args):
    return spread(plan, *args)


def spread(plan, queries, keys, values, doc_lengths):
    kv = pack(pack_kv_kernel, (8, 2, ROWS, HD), keys, values)
    own = lax.all_to_all(kv, PLANE, split_axis=0, concat_axis=0, tiled=True)
    q = pack(pack_q_kernel, (8, HEADS, ROWS, HD), queries)
    q = lax.all_to_all(q, PLANE, split_axis=0, concat_axis=0, tiled=True)

    held = {0: (own[None], 0)}
    for name, sent, got, _ in STEPS:
        parts = [held[s][0][held[s][1]] for s in sent]
        back = lax.ppermute(jnp.stack(parts), RING, plan.pairs[name])
        for i, s in enumerate(got):
            held[s] = (back, i)

    heads_in, state = (doc_lengths, q), None
    for j, call in enumerate(CALLS):
        state = attend(heads_in, call, [held[s] for s in call], state, j == len(CALLS) - 1)
        if j == 0:
            heads_in, state = state[:2], state[2:]
    out = lax.all_to_all(state, PLANE, split_axis=0, concat_axis=0, tiled=True)
    return jnp.transpose(out, (2, 0, 1, 3)).reshape(1, ROWS, 32 * HD)


def solution(mesh):
    fine = Mesh(mesh.devices.reshape(4, 2, 4, 16, 2), AXES)
    spec = P(("y", "zl", "c"), ("x", "zh"), None)
    return jax.shard_map(
        functools.partial(body, Plan(4, 16, 2)),
        mesh=fine,
        in_specs=(spec, spec, spec, P()),
        out_specs=spec,
        check_vma=False,
    )
```

```python
import functools
import math

import jax
import jax.numpy as jnp
from jax import lax
from jax.experimental import pallas as pl
from jax.experimental.pallas import tpu as pltpu
from jax.sharding import Mesh
from jax.sharding import PartitionSpec as P


HD = 128
ROWS = 32
HEADS = 4
CHUNK = 64
NEG_FILL = -1e30
AXES = ("x", "zh", "y", "zl", "c")
PLANE = ("x", "c")
RING = ("zh", "y", "zl")

STEPS = (
    ("m1", (0,), (-9,), -9),
    ("p1", (0,), (3,), 3),
    ("p2", (3,), (6,), 3),
    ("e1", (0, 3), (1, 4), 1),
    ("m2", (-9,), (-12,), -3),
    ("e2", (6, -9), (7, -8), 1),
    ("m3", (-12,), (-15,), -3),
    ("g2", (1, 4, 7, -12), (2, 5, 8, -11), 1),
    ("g1", (-9, -12), (-10, -13), -1),
    ("h2", (-15,), (-14,), 1),
    ("h1", (-15,), (-16,), -1),
)
CALLS = (
    (0, 3, 6),
    (1, 4, 7, -8, -9, -12),
    (2, 5, 8, -10, -11, -13, -15),
    (-14, -16),
)


class Plan:
    def __init__(self, outer, half, halves):
        length, chips = half * halves, outer * half
        index = lambda z, y: ((z // half) * outer + y) * half + z % half
        where = {(z, y * half + z % half): index(z, y) for z in range(length) for y in range(outer)}
        held = {0: {key: key for key in where}}
        moves = {}
        for name, sent, got, shift in STEPS:
            target = {}
            for slot, new in zip(sent, got):
                held[new] = {}
                for (z, n), (zs, ns) in held[slot].items():
                    z2 = (z + shift) % length
                    to = (z2, (ns + (z2 - zs) % half) % chips)
                    assert target.setdefault((z, n), to) == to
                    held[new][to] = (zs, ns)
            assert len(set(target.values())) == len(target)
            moves[name] = target
        wanted = {s: {key for key in where if at[key][1] <= key[1]} for s, at in held.items()}
        self.pairs = {}
        for name, sent, got, shift in reversed(STEPS):
            used = {a: b for a, b in moves[name].items() if any(b in wanted[s] for s in got)}
            for slot, new in zip(sent, got):
                wanted[slot] |= {a for a, b in used.items() if b in wanted[new]}
            self.pairs[name] = [(where[a], where[b]) for a, b in sorted(used.items())]
        for (z, n) in where:
            want = {(h * half + m % half, m) for m in range(max(0, n - half // 2), n + 1) for h in range(halves)}
            got = [held[s][z, n] for call in CALLS for s in call]
            assert len(set(got)) == len(got) and want <= set(got)


def row_offsets(shape, dim):
    i = lax.broadcasted_iota(jnp.int32, shape, dim)
    return ((i >> 5) & 1) * 256 + (i >> 6) * 64 + (i & 31)


def document_bounds(lengths):
    count = lengths.shape[0]
    lane = lax.broadcasted_iota(jnp.int32, (1, HD), 1)
    begin = jnp.where(lane == count, -(1 << 24), 1 << 24)
    end = jnp.where(lane == count, 0, -(1 << 24))
    at = jnp.int32(0)
    for d in range(count):
        begin = jnp.where(lane == d, at, begin)
        at = at + lengths[d]
        end = jnp.where(lane == d, at, end)
    return begin, end


def attend_kernel(slots, first, last, *refs):
    count = len(slots)
    refs = list(refs)
    arrays = max(a for _, a, _ in slots) + 1
    if first:
        lengths, q_ref, *refs = refs
    else:
        bounds, q_all, top_in, acc_in, *refs = refs
    kv, refs = refs[:arrays], refs[arrays:]
    if last:
        out_ref, tops, *refs = refs
    elif first:
        bounds, q_all, tops, acc_out, *refs = refs
    else:
        tops, acc_out, *refs = refs
    k_all, v_all, *refs = refs
    scores, rounded = refs[:2], refs[2:]
    unit = math.log2(math.e) / math.sqrt(HD)
    half, halves = lax.axis_size("zl"), lax.axis_size("zh")

    chip = lax.axis_index("y") * half + lax.axis_index("zl")
    zh = lax.axis_index("zh")
    offsets = row_offsets((256, HD), 0)

    def members(base):
        return (offsets >= bounds[0:1] - base) & (offsets < bounds[1:2] - base)

    if first:
        begin, end = document_bounds(lengths)
        bounds[0:1], bounds[1:2] = begin, end
        apart = jnp.where(members(chip * 512 + zh * ROWS), 0.0, NEG_FILL).astype(jnp.bfloat16)
        for h in range(HEADS):
            q_all[h, :, :HD] = q_ref[:, h].reshape(256, HD)
            q_all[h, :, HD:] = apart

    later = {}
    for j, (slot, a, i) in enumerate(slots):
        rows = slice(j * 256, (j + 1) * 256)
        back = slot if slot >= 0 else slot + half
        from_zh = ((zh * half + lax.axis_index("zl") - slot + half * halves) >> 4) & 1
        base = (chip - back) * 512 + from_zh * ROWS
        k_all[rows, :HD] = kv[a][i, :, 0].reshape(256, HD)
        k_all[rows, HD:] = jnp.where(members(base), 1.0, 0.0).astype(jnp.bfloat16)
        v_all[rows, :HD] = kv[a][i, :, 1].reshape(256, HD)
        if back == 0:
            later[j] = (from_zh - zh) * ROWS
    v_all[:, HD:] = jnp.ones((count * 256, HD), jnp.bfloat16)

    def score(h):
        scores[h & 1][...] = lax.dot_general(
            q_all[h], k_all[...], (((1,), (1,)), ((), ())), preferred_element_type=jnp.float32
        )

    def weigh(h):
        for r in range(0, 256, CHUNK):
            rows = slice(r, r + CHUNK)
            wide = None
            for j in range(count):
                cols = slice(j * 256, (j + 1) * 256)
                s = scores[h & 1][rows, cols]
                if j in later:
                    q_at = row_offsets((256, 1), 0)[rows] - later[j]
                    s = jnp.where(row_offsets((1, 256), 1) <= q_at, s, NEG_FILL)
                    scores[h & 1][rows, cols] = s
                wide = s if wide is None else jnp.maximum(wide, s)
            top = jnp.max(wide, axis=1, keepdims=True)
            if not first:
                top = jnp.maximum(top_in[h, rows], top)
            for j in range(count):
                cols = slice(j * 256, (j + 1) * 256)
                w = jnp.exp2((scores[h & 1][rows, cols] - top) * unit)
                rounded[h & 1][rows, cols] = w.astype(jnp.bfloat16)
            tops[h, rows] = top

    def gather(h):
        for r in range(0, 256, 128):
            rows = slice(r, r + 128)
            added = jnp.dot(rounded[h & 1][rows], v_all[...], preferred_element_type=jnp.float32)
            if not first:
                factor = jnp.exp2((top_in[h, rows] - tops[h, rows]) * unit)
                added = added + acc_in[h, rows] * factor
            if last:
                res = added[:, :HD] / added[:, HD:]
                out_ref[r // ROWS : r // ROWS + 4, h] = res.astype(jnp.bfloat16).reshape(4, ROWS, HD)
            else:
                acc_out[h, rows] = added

    for h in range(HEADS + 2):
        if h < HEADS:
            score(h)
        if h >= 2:
            gather(h - 2)
        if 1 <= h <= HEADS:
            weigh(h - 1)


VMEM = pl.BlockSpec(memory_space=pltpu.VMEM)
SMEM = pl.BlockSpec(memory_space=pltpu.SMEM)


def attend(heads_in, slots, blocks, state, last):
    n = len(blocks)
    first = state is None
    bounds = jax.ShapeDtypeStruct((8, HD), jnp.int32)
    q_all = jax.ShapeDtypeStruct((HEADS, 256, 2 * HD), jnp.bfloat16)
    top = jax.ShapeDtypeStruct((HEADS, 256, 1), jnp.float32)
    acc = jax.ShapeDtypeStruct((HEADS, 256, 2 * HD), jnp.float32)
    out = jax.ShapeDtypeStruct((8, HEADS, ROWS, HD), jnp.bfloat16)
    outs = out if last else (bounds, q_all, top, acc) if first else (top, acc)
    arrays = list({id(b): b for b, _ in blocks}.values())
    number = {id(b): a for a, b in enumerate(arrays)}
    where = tuple((s, number[id(b)], i) for s, (b, i) in zip(slots, blocks))
    return pl.pallas_call(
        functools.partial(attend_kernel, where, first, last),
        out_shape=outs,
        in_specs=([SMEM, VMEM] if first else [VMEM] * 4) + [VMEM] * len(arrays),
        out_specs=VMEM if last else tuple(VMEM for _ in outs),
        scratch_shapes=([pltpu.VMEM(top.shape, top.dtype)] if last else [])
        + [
            pltpu.VMEM((n * 256, 2 * HD), jnp.bfloat16),
            pltpu.VMEM((n * 256, 2 * HD), jnp.bfloat16),
            pltpu.VMEM((256, n * 256), jnp.float32),
            pltpu.VMEM((256, n * 256), jnp.float32),
            pltpu.VMEM((256, n * 256), jnp.bfloat16),
            pltpu.VMEM((256, n * 256), jnp.bfloat16),
        ],
        compiler_params=pltpu.CompilerParams(vmem_limit_bytes=(6 + 2 * n) << 20),
        cost_estimate=pl.CostEstimate(
            flops=n * HEADS * 256 * 256 * HD * 4,
            bytes_accessed=n * 131072 + 1500000,
            transcendentals=n * HEADS * 256 * 256,
        ),
    )(*heads_in, *(() if first else state), *arrays)


def pack_kv_kernel(k_ref, v_ref, out_ref):
    for g in range(8):
        out_ref[g, 0] = k_ref[0, :, g * HD : (g + 1) * HD]
        out_ref[g, 1] = v_ref[0, :, g * HD : (g + 1) * HD]


def pack_q_kernel(q_ref, out_ref):
    for g in range(8):
        for h in range(HEADS):
            at = (g * HEADS + h) * HD
            out_ref[g, h] = q_ref[0, :, at : at + HD]


def pack(kernel, shape, *arrays):
    return pl.pallas_call(
        kernel,
        out_shape=jax.ShapeDtypeStruct(shape, jnp.bfloat16),
        in_specs=[VMEM] * len(arrays),
        out_specs=VMEM,
    )(*arrays)


def body(plan, *args):
    return spread(plan, *args)


def spread(plan, queries, keys, values, doc_lengths):
    kv = pack(pack_kv_kernel, (8, 2, ROWS, HD), keys, values)
    own = lax.all_to_all(kv, PLANE, split_axis=0, concat_axis=0, tiled=True)
    q = pack(pack_q_kernel, (8, HEADS, ROWS, HD), queries)
    q = lax.all_to_all(q, PLANE, split_axis=0, concat_axis=0, tiled=True)

    held = {0: (own[None], 0)}
    for name, sent, got, _ in STEPS:
        parts = [held[s][0][held[s][1]] for s in sent]
        if len(parts) > 1:
            parts = lax.optimization_barrier(parts)
        back = lax.ppermute(jnp.stack(parts), RING, plan.pairs[name])
        for i, s in enumerate(got):
            held[s] = (back, i)

    heads_in, state = (doc_lengths, q), None
    for j, call in enumerate(CALLS):
        state = attend(heads_in, call, [held[s] for s in call], state, j == len(CALLS) - 1)
        if j == 0:
            heads_in, state = state[:2], state[2:]
    out = lax.all_to_all(state, PLANE, split_axis=0, concat_axis=0, tiled=True)
    return jnp.transpose(out, (2, 0, 1, 3)).reshape(1, ROWS, 32 * HD)


def solution(mesh):
    fine = Mesh(mesh.devices.reshape(4, 2, 4, 16, 2), AXES)
    spec = P(("y", "zl", "c"), ("x", "zh"), None)
    return jax.shard_map(
        functools.partial(body, Plan(4, 16, 2)),
        mesh=fine,
        in_specs=(spec, spec, spec, P()),
        out_specs=spec,
        check_vma=False,
    )
```

```python
import functools
import math

import jax
import jax.numpy as jnp
from jax import lax
from jax.experimental import pallas as pl
from jax.experimental.pallas import tpu as pltpu
from jax.sharding import Mesh
from jax.sharding import PartitionSpec as P


HD = 128
ROWS = 32
HEADS = 4
CHUNK = 64
NEG_FILL = -1e30
AXES = ("x", "zh", "y", "zl", "c")
PLANE = ("x", "c")
RING = ("zh", "y", "zl")

STEPS = (
    ("m1", (0,), (-9,), -9),
    ("p1", (0,), (3,), 3),
    ("p2", (3,), (6,), 3),
    ("e1", (0, 3), (1, 4), 1),
    ("m2", (-9,), (-12,), -3),
    ("e2", (6, -9), (7, -8), 1),
    ("m3", (-12,), (-15,), -3),
    ("g2", (1, 4, 7, -12), (2, 5, 8, -11), 1),
    ("g1", (-9, -12), (-10, -13), -1),
    ("h2", (-15,), (-14,), 1),
    ("h1", (-15,), (-16,), -1),
)
CALLS = (
    (0, 3, 6, -9),
    (1, 4, 7, -8, -12),
    (2, 5, 8, -10, -11, -13, -15),
    (-14, -16),
)


class Plan:
    def __init__(self, outer, half, halves):
        length, chips = half * halves, outer * half
        index = lambda z, y: ((z // half) * outer + y) * half + z % half
        where = {(z, y * half + z % half): index(z, y) for z in range(length) for y in range(outer)}
        held = {0: {key: key for key in where}}
        moves = {}
        for name, sent, got, shift in STEPS:
            target = {}
            for slot, new in zip(sent, got):
                held[new] = {}
                for (z, n), (zs, ns) in held[slot].items():
                    z2 = (z + shift) % length
                    to = (z2, (ns + (z2 - zs) % half) % chips)
                    assert target.setdefault((z, n), to) == to
                    held[new][to] = (zs, ns)
            assert len(set(target.values())) == len(target)
            moves[name] = target
        wanted = {s: {key for key in where if at[key][1] <= key[1]} for s, at in held.items()}
        self.pairs = {}
        for name, sent, got, shift in reversed(STEPS):
            used = {a: b for a, b in moves[name].items() if any(b in wanted[s] for s in got)}
            for slot, new in zip(sent, got):
                wanted[slot] |= {a for a, b in used.items() if b in wanted[new]}
            self.pairs[name] = [(where[a], where[b]) for a, b in sorted(used.items())]
        for (z, n) in where:
            want = {(h * half + m % half, m) for m in range(max(0, n - half // 2), n + 1) for h in range(halves)}
            got = [held[s][z, n] for call in CALLS for s in call]
            assert len(set(got)) == len(got) and want <= set(got)


def row_offsets(shape, dim):
    i = lax.broadcasted_iota(jnp.int32, shape, dim)
    return ((i >> 5) & 1) * 256 + (i >> 6) * 64 + (i & 31)


def document_bounds(lengths):
    count = lengths.shape[0]
    lane = lax.broadcasted_iota(jnp.int32, (1, HD), 1)
    begin = jnp.where(lane == count, -(1 << 24), 1 << 24)
    end = jnp.where(lane == count, 0, -(1 << 24))
    at = jnp.int32(0)
    for d in range(count):
        begin = jnp.where(lane == d, at, begin)
        at = at + lengths[d]
        end = jnp.where(lane == d, at, end)
    return begin, end


def attend_kernel(slots, first, last, *refs):
    count = len(slots)
    refs = list(refs)
    arrays = max(a for _, a, _ in slots) + 1
    if first:
        lengths, q_ref, *refs = refs
    else:
        bounds, q_all, top_in, acc_in, *refs = refs
    kv, refs = refs[:arrays], refs[arrays:]
    if last:
        out_ref, tops, *refs = refs
    elif first:
        bounds, q_all, tops, acc_out, *refs = refs
    else:
        tops, acc_out, *refs = refs
    k_all, v_all, *refs = refs
    scores, rounded = refs[:2], refs[2:]
    unit = math.log2(math.e) / math.sqrt(HD)
    half, halves = lax.axis_size("zl"), lax.axis_size("zh")

    chip = lax.axis_index("y") * half + lax.axis_index("zl")
    zh = lax.axis_index("zh")
    offsets = row_offsets((256, HD), 0)

    def members(base):
        return (offsets >= bounds[0:1] - base) & (offsets < bounds[1:2] - base)

    if first:
        begin, end = document_bounds(lengths)
        bounds[0:1], bounds[1:2] = begin, end
        apart = jnp.where(members(chip * 512 + zh * ROWS), 0.0, NEG_FILL).astype(jnp.bfloat16)
        for h in range(HEADS):
            q_all[h, :, :HD] = q_ref[:, h].reshape(256, HD)
            q_all[h, :, HD:] = apart

    def run():
        later = {}
        for j, (slot, a, i) in enumerate(slots):
            rows = slice(j * 256, (j + 1) * 256)
            back = slot if slot >= 0 else slot + half
            from_zh = ((zh * half + lax.axis_index("zl") - slot + half * halves) >> 4) & 1
            base = (chip - back) * 512 + from_zh * ROWS
            k_all[rows, :HD] = kv[a][i, :, 0].reshape(256, HD)
            k_all[rows, HD:] = jnp.where(members(base), 1.0, 0.0).astype(jnp.bfloat16)
            v_all[rows, :HD] = kv[a][i, :, 1].reshape(256, HD)
            if back == 0:
                later[j] = (from_zh - zh) * ROWS
        v_all[:, HD:] = jnp.ones((count * 256, HD), jnp.bfloat16)

        def score(h):
            scores[h & 1][...] = lax.dot_general(
                q_all[h], k_all[...], (((1,), (1,)), ((), ())), preferred_element_type=jnp.float32
            )

        def weigh(h):
            for r in range(0, 256, CHUNK):
                rows = slice(r, r + CHUNK)
                wide = None
                for j in range(count):
                    cols = slice(j * 256, (j + 1) * 256)
                    s = scores[h & 1][rows, cols]
                    if j in later:
                        q_at = row_offsets((256, 1), 0)[rows] - later[j]
                        s = jnp.where(row_offsets((1, 256), 1) <= q_at, s, NEG_FILL)
                        scores[h & 1][rows, cols] = s
                    wide = s if wide is None else jnp.maximum(wide, s)
                top = jnp.max(wide, axis=1, keepdims=True)
                if not first:
                    top = jnp.maximum(top_in[h, rows], top)
                for j in range(count):
                    cols = slice(j * 256, (j + 1) * 256)
                    w = jnp.exp2((scores[h & 1][rows, cols] - top) * unit)
                    rounded[h & 1][rows, cols] = w.astype(jnp.bfloat16)
                tops[h, rows] = top

        def gather(h):
            for r in range(0, 256, 128):
                rows = slice(r, r + 128)
                added = jnp.dot(rounded[h & 1][rows], v_all[...], preferred_element_type=jnp.float32)
                if not first:
                    factor = jnp.exp2((top_in[h, rows] - tops[h, rows]) * unit)
                    added = added + acc_in[h, rows] * factor
                if last:
                    res = added[:, :HD] / added[:, HD:]
                    out_ref[r // ROWS : r // ROWS + 4, h] = res.astype(jnp.bfloat16).reshape(4, ROWS, HD)
                else:
                    acc_out[h, rows] = added

        for h in range(HEADS + 2):
            if h < HEADS:
                score(h)
            if h >= 2:
                gather(h - 2)
            if 1 <= h <= HEADS:
                weigh(h - 1)

    nearest = min(s if s >= 0 else s + half for s, _, _ in slots)
    if first or last or nearest == 0:
        run()
        return
    pl.when(chip >= nearest)(run)

    @pl.when(chip < nearest)
    def _():
        tops[...] = top_in[...]
        acc_out[...] = acc_in[...]


VMEM = pl.BlockSpec(memory_space=pltpu.VMEM)
SMEM = pl.BlockSpec(memory_space=pltpu.SMEM)


def attend(heads_in, slots, blocks, state, last):
    n = len(blocks)
    first = state is None
    bounds = jax.ShapeDtypeStruct((8, HD), jnp.int32)
    q_all = jax.ShapeDtypeStruct((HEADS, 256, 2 * HD), jnp.bfloat16)
    top = jax.ShapeDtypeStruct((HEADS, 256, 1), jnp.float32)
    acc = jax.ShapeDtypeStruct((HEADS, 256, 2 * HD), jnp.float32)
    out = jax.ShapeDtypeStruct((8, HEADS, ROWS, HD), jnp.bfloat16)
    outs = out if last else (bounds, q_all, top, acc) if first else (top, acc)
    arrays = list({id(b): b for b, _ in blocks}.values())
    number = {id(b): a for a, b in enumerate(arrays)}
    where = tuple((s, number[id(b)], i) for s, (b, i) in zip(slots, blocks))
    return pl.pallas_call(
        functools.partial(attend_kernel, where, first, last),
        out_shape=outs,
        in_specs=([SMEM, VMEM] if first else [VMEM] * 4) + [VMEM] * len(arrays),
        out_specs=VMEM if last else tuple(VMEM for _ in outs),
        scratch_shapes=([pltpu.VMEM(top.shape, top.dtype)] if last else [])
        + [
            pltpu.VMEM((n * 256, 2 * HD), jnp.bfloat16),
            pltpu.VMEM((n * 256, 2 * HD), jnp.bfloat16),
            pltpu.VMEM((256, n * 256), jnp.float32),
            pltpu.VMEM((256, n * 256), jnp.float32),
            pltpu.VMEM((256, n * 256), jnp.bfloat16),
            pltpu.VMEM((256, n * 256), jnp.bfloat16),
        ],
        compiler_params=pltpu.CompilerParams(vmem_limit_bytes=(6 + 2 * n) << 20),
        cost_estimate=pl.CostEstimate(
            flops=n * HEADS * 256 * 256 * HD * 4,
            bytes_accessed=n * 131072 + 1500000,
            transcendentals=n * HEADS * 256 * 256,
        ),
    )(*heads_in, *(() if first else state), *arrays)


def copy_all(copies):
    for c in copies:
        c.start()
    for c in copies:
        c.wait()


def unpack_kernel(in_ref, out_ref, sems):
    copy_all(
        [
            pltpu.make_async_copy(
                in_ref.at[i // HEADS, i % HEADS],
                out_ref.at[0, :, i * HD : (i + 1) * HD],
                sems.at[i],
            )
            for i in range(8 * HEADS)
        ]
    )


def unpack(array):
    return pl.pallas_call(
        unpack_kernel,
        out_shape=jax.ShapeDtypeStruct((1, ROWS, 8 * HEADS * HD), jnp.bfloat16),
        in_specs=[VMEM],
        out_specs=pl.BlockSpec(memory_space=pltpu.HBM),
        scratch_shapes=[pltpu.SemaphoreType.DMA((8 * HEADS,))],
        compiler_params=pltpu.CompilerParams(vmem_limit_bytes=4 << 20),
    )(array)


def pack_kv_kernel(k_ref, v_ref, out_ref):
    for g in range(8):
        out_ref[g, 0] = k_ref[0, :, g * HD : (g + 1) * HD]
        out_ref[g, 1] = v_ref[0, :, g * HD : (g + 1) * HD]


def pack_q_kernel(q_ref, out_ref):
    for g in range(8):
        for h in range(HEADS):
            at = (g * HEADS + h) * HD
            out_ref[g, h] = q_ref[0, :, at : at + HD]


def pack(kernel, shape, *arrays):
    return pl.pallas_call(
        kernel,
        out_shape=jax.ShapeDtypeStruct(shape, jnp.bfloat16),
        in_specs=[VMEM] * len(arrays),
        out_specs=VMEM,
    )(*arrays)


def body(plan, *args):
    return spread(plan, *args)


def spread(plan, queries, keys, values, doc_lengths):
    kv = pack(pack_kv_kernel, (8, 2, ROWS, HD), keys, values)
    own = lax.all_to_all(kv, PLANE, split_axis=0, concat_axis=0, tiled=True)
    q = pack(pack_q_kernel, (8, HEADS, ROWS, HD), queries)
    q = lax.all_to_all(q, PLANE, split_axis=0, concat_axis=0, tiled=True)

    held = {0: (own[None], 0)}
    for name, sent, got, _ in STEPS:
        parts = [held[s][0][held[s][1]] for s in sent]
        if len(parts) > 1:
            parts = lax.optimization_barrier(parts)
        back = lax.ppermute(jnp.stack(parts), RING, plan.pairs[name])
        for i, s in enumerate(got):
            held[s] = (back, i)

    heads_in, state = (doc_lengths, q), None
    for j, call in enumerate(CALLS):
        state = attend(heads_in, call, [held[s] for s in call], state, j == len(CALLS) - 1)
        if j == 0:
            heads_in, state = state[:2], state[2:]
    out = lax.all_to_all(state, PLANE, split_axis=0, concat_axis=0, tiled=True)
    return unpack(out)


def solution(mesh):
    fine = Mesh(mesh.devices.reshape(4, 2, 4, 16, 2), AXES)
    spec = P(("y", "zl", "c"), ("x", "zh"), None)
    return jax.shard_map(
        functools.partial(body, Plan(4, 16, 2)),
        mesh=fine,
        in_specs=(spec, spec, spec, P()),
        out_specs=spec,
        check_vma=False,
    )
```

```python
import functools
import math

import jax
import jax.numpy as jnp
from jax import lax
from jax.experimental import pallas as pl
from jax.experimental.pallas import tpu as pltpu
from jax.sharding import Mesh
from jax.sharding import PartitionSpec as P


HD = 128
ROWS = 32
HEADS = 4
CHUNK = 64
NEG_FILL = -1e30
AXES = ("x", "zh", "y", "zl", "c")
PLANE = ("x", "c")
RING = ("zh", "y", "zl")

STEPS = (
    ("m1", (0,), (-9,), -9),
    ("p1", (0,), (3,), 3),
    ("p2", (3,), (6,), 3),
    ("e1", (0, 3), (1, 4), 1),
    ("m2", (-9,), (-12,), -3),
    ("e2", (6, -9), (7, -8), 1),
    ("m3", (-12,), (-15,), -3),
    ("g2", (1, 4, 7, -12), (2, 5, 8, -11), 1),
    ("g1", (-9, -12), (-10, -13), -1),
    ("h2", (-15,), (-14,), 1),
    ("h1", (-15,), (-16,), -1),
)
CALLS = (
    (0, 3, 6, 1, 4, -9),
    (7, -8, -12, 2, 5, 8, -10, -11, -13, -15),
    (-14, -16),
)


class Plan:
    def __init__(self, outer, half, halves):
        length, chips = half * halves, outer * half
        index = lambda z, y: ((z // half) * outer + y) * half + z % half
        where = {(z, y * half + z % half): index(z, y) for z in range(length) for y in range(outer)}
        held = {0: {key: key for key in where}}
        moves = {}
        for name, sent, got, shift in STEPS:
            target = {}
            for slot, new in zip(sent, got):
                held[new] = {}
                for (z, n), (zs, ns) in held[slot].items():
                    z2 = (z + shift) % length
                    to = (z2, (ns + (z2 - zs) % half) % chips)
                    assert target.setdefault((z, n), to) == to
                    held[new][to] = (zs, ns)
            assert len(set(target.values())) == len(target)
            moves[name] = target
        wanted = {s: {key for key in where if at[key][1] <= key[1]} for s, at in held.items()}
        self.pairs = {}
        for name, sent, got, shift in reversed(STEPS):
            used = {a: b for a, b in moves[name].items() if any(b in wanted[s] for s in got)}
            for slot, new in zip(sent, got):
                wanted[slot] |= {a for a, b in used.items() if b in wanted[new]}
            self.pairs[name] = [(where[a], where[b]) for a, b in sorted(used.items())]
        for (z, n) in where:
            want = {(h * half + m % half, m) for m in range(max(0, n - half // 2), n + 1) for h in range(halves)}
            got = [held[s][z, n] for call in CALLS for s in call]
            assert len(set(got)) == len(got) and want <= set(got)


def row_offsets(shape, dim):
    i = lax.broadcasted_iota(jnp.int32, shape, dim)
    return ((i >> 5) & 1) * 256 + (i >> 6) * 64 + (i & 31)


def document_bounds(lengths):
    count = lengths.shape[0]
    lane = lax.broadcasted_iota(jnp.int32, (1, HD), 1)
    begin = jnp.where(lane == count, -(1 << 24), 1 << 24)
    end = jnp.where(lane == count, 0, -(1 << 24))
    at = jnp.int32(0)
    for d in range(count):
        begin = jnp.where(lane == d, at, begin)
        at = at + lengths[d]
        end = jnp.where(lane == d, at, end)
    return begin, end


def attend_kernel(slots, first, last, *refs):
    count = len(slots)
    refs = list(refs)
    arrays = max(a for _, a, _ in slots) + 1
    if first:
        lengths, q_ref, *refs = refs
    else:
        bounds, q_all, top_in, acc_in, *refs = refs
    kv, refs = refs[:arrays], refs[arrays:]
    if last:
        out_ref, tops, *refs = refs
    elif first:
        bounds, q_all, tops, acc_out, *refs = refs
    else:
        tops, acc_out, *refs = refs
    k_all, v_all, *refs = refs
    scores, rounded = refs[:2], refs[2:]
    unit = math.log2(math.e) / math.sqrt(HD)
    half, halves = lax.axis_size("zl"), lax.axis_size("zh")

    chip = lax.axis_index("y") * half + lax.axis_index("zl")
    zh = lax.axis_index("zh")
    offsets = row_offsets((256, HD), 0)

    def members(base):
        return (offsets >= bounds[0:1] - base) & (offsets < bounds[1:2] - base)

    if first:
        begin, end = document_bounds(lengths)
        bounds[0:1], bounds[1:2] = begin, end
        apart = jnp.where(members(chip * 512 + zh * ROWS), 0.0, NEG_FILL).astype(jnp.bfloat16)
        for h in range(HEADS):
            q_all[h, :, :HD] = q_ref[:, h].reshape(256, HD)
            q_all[h, :, HD:] = apart

    def run():
        later = {}
        for j, (slot, a, i) in enumerate(slots):
            rows = slice(j * 256, (j + 1) * 256)
            back = slot if slot >= 0 else slot + half
            from_zh = ((zh * half + lax.axis_index("zl") - slot + half * halves) >> 4) & 1
            base = (chip - back) * 512 + from_zh * ROWS
            k_all[rows, :HD] = kv[a][i, :, 0].reshape(256, HD)
            k_all[rows, HD:] = jnp.where(members(base), 1.0, 0.0).astype(jnp.bfloat16)
            v_all[rows, :HD] = kv[a][i, :, 1].reshape(256, HD)
            if back == 0:
                later[j] = (from_zh - zh) * ROWS
        v_all[:, HD:] = jnp.ones((count * 256, HD), jnp.bfloat16)

        def score(h):
            scores[h & 1][...] = lax.dot_general(
                q_all[h], k_all[...], (((1,), (1,)), ((), ())), preferred_element_type=jnp.float32
            )

        def weigh(h):
            for r in range(0, 256, CHUNK):
                rows = slice(r, r + CHUNK)
                wide = None
                for j in range(count):
                    cols = slice(j * 256, (j + 1) * 256)
                    s = scores[h & 1][rows, cols]
                    if j in later:
                        q_at = row_offsets((256, 1), 0)[rows] - later[j]
                        s = jnp.where(row_offsets((1, 256), 1) <= q_at, s, NEG_FILL)
                        scores[h & 1][rows, cols] = s
                    wide = s if wide is None else jnp.maximum(wide, s)
                top = jnp.max(wide, axis=1, keepdims=True)
                if not first:
                    top = jnp.maximum(top_in[h, rows], top)
                for j in range(count):
                    cols = slice(j * 256, (j + 1) * 256)
                    w = jnp.exp2((scores[h & 1][rows, cols] - top) * unit)
                    rounded[h & 1][rows, cols] = w.astype(jnp.bfloat16)
                tops[h, rows] = top

        def gather(h):
            for r in range(0, 256, 128):
                rows = slice(r, r + 128)
                added = jnp.dot(rounded[h & 1][rows], v_all[...], preferred_element_type=jnp.float32)
                if not first:
                    factor = jnp.exp2((top_in[h, rows] - tops[h, rows]) * unit)
                    added = added + acc_in[h, rows] * factor
                if last:
                    res = added[:, :HD] / added[:, HD:]
                    out_ref[r // ROWS : r // ROWS + 4, h] = res.astype(jnp.bfloat16).reshape(4, ROWS, HD)
                else:
                    acc_out[h, rows] = added

        for h in range(HEADS + 2):
            if h < HEADS:
                score(h)
            if h >= 2:
                gather(h - 2)
            if 1 <= h <= HEADS:
                weigh(h - 1)

    nearest = min(s if s >= 0 else s + half for s, _, _ in slots)
    if first or last or nearest == 0:
        run()
        return
    pl.when(chip >= nearest)(run)

    @pl.when(chip < nearest)
    def _():
        tops[...] = top_in[...]
        acc_out[...] = acc_in[...]


VMEM = pl.BlockSpec(memory_space=pltpu.VMEM)
SMEM = pl.BlockSpec(memory_space=pltpu.SMEM)


def attend(heads_in, slots, blocks, state, last):
    n = len(blocks)
    first = state is None
    bounds = jax.ShapeDtypeStruct((8, HD), jnp.int32)
    q_all = jax.ShapeDtypeStruct((HEADS, 256, 2 * HD), jnp.bfloat16)
    top = jax.ShapeDtypeStruct((HEADS, 256, 1), jnp.float32)
    acc = jax.ShapeDtypeStruct((HEADS, 256, 2 * HD), jnp.float32)
    out = jax.ShapeDtypeStruct((8, HEADS, ROWS, HD), jnp.bfloat16)
    outs = out if last else (bounds, q_all, top, acc) if first else (top, acc)
    arrays = list({id(b): b for b, _ in blocks}.values())
    number = {id(b): a for a, b in enumerate(arrays)}
    where = tuple((s, number[id(b)], i) for s, (b, i) in zip(slots, blocks))
    return pl.pallas_call(
        functools.partial(attend_kernel, where, first, last),
        out_shape=outs,
        in_specs=([SMEM, VMEM] if first else [VMEM] * 4) + [VMEM] * len(arrays),
        out_specs=VMEM if last else tuple(VMEM for _ in outs),
        scratch_shapes=([pltpu.VMEM(top.shape, top.dtype)] if last else [])
        + [
            pltpu.VMEM((n * 256, 2 * HD), jnp.bfloat16),
            pltpu.VMEM((n * 256, 2 * HD), jnp.bfloat16),
            pltpu.VMEM((256, n * 256), jnp.float32),
            pltpu.VMEM((256, n * 256), jnp.float32),
            pltpu.VMEM((256, n * 256), jnp.bfloat16),
            pltpu.VMEM((256, n * 256), jnp.bfloat16),
        ],
        compiler_params=pltpu.CompilerParams(vmem_limit_bytes=(6 + 2 * n) << 20),
        cost_estimate=pl.CostEstimate(
            flops=n * HEADS * 256 * 256 * HD * 4,
            bytes_accessed=n * 131072 + 1500000,
            transcendentals=n * HEADS * 256 * 256,
        ),
    )(*heads_in, *(() if first else state), *arrays)


def copy_all(copies):
    for c in copies:
        c.start()
    for c in copies:
        c.wait()


def pack_kv_kernel(k_ref, v_ref, out_ref, sems):
    copy_all(
        [
            pltpu.make_async_copy(
                ref.at[0, :, g * HD : (g + 1) * HD], out_ref.at[g, part], sems.at[2 * g + part]
            )
            for g in range(8)
            for part, ref in enumerate((k_ref, v_ref))
        ]
    )


def pack_q_kernel(q_ref, out_ref, sems):
    copy_all(
        [
            pltpu.make_async_copy(
                q_ref.at[0, :, i * HD : (i + 1) * HD],
                out_ref.at[i // HEADS, i % HEADS],
                sems.at[i],
            )
            for i in range(8 * HEADS)
        ]
    )


def unpack_kernel(in_ref, out_ref, sems):
    copy_all(
        [
            pltpu.make_async_copy(
                in_ref.at[i // HEADS, i % HEADS],
                out_ref.at[0, :, i * HD : (i + 1) * HD],
                sems.at[i],
            )
            for i in range(8 * HEADS)
        ]
    )


def unpack(array):
    return pl.pallas_call(
        unpack_kernel,
        out_shape=jax.ShapeDtypeStruct((1, ROWS, 8 * HEADS * HD), jnp.bfloat16),
        in_specs=[VMEM],
        out_specs=pl.BlockSpec(memory_space=pltpu.HBM),
        scratch_shapes=[pltpu.SemaphoreType.DMA((8 * HEADS,))],
        compiler_params=pltpu.CompilerParams(vmem_limit_bytes=4 << 20),
    )(array)


def pack(kernel, shape, *arrays):
    return pl.pallas_call(
        kernel,
        out_shape=jax.ShapeDtypeStruct(shape, jnp.bfloat16),
        in_specs=[pl.BlockSpec(memory_space=pltpu.HBM)] * len(arrays),
        out_specs=VMEM,
        scratch_shapes=[pltpu.SemaphoreType.DMA((shape[0] * shape[1],))],
        compiler_params=pltpu.CompilerParams(vmem_limit_bytes=4 << 20),
    )(*[pltpu.with_memory_space_constraint(a, pltpu.HBM) for a in arrays])


def body(plan, *args):
    return spread(plan, *args)


def spread(plan, queries, keys, values, doc_lengths):
    kv = pack(pack_kv_kernel, (8, 2, ROWS, HD), keys, values)
    own = lax.all_to_all(kv, PLANE, split_axis=0, concat_axis=0, tiled=True)
    q = pack(pack_q_kernel, (8, HEADS, ROWS, HD), queries)
    q = lax.all_to_all(q, PLANE, split_axis=0, concat_axis=0, tiled=True)

    held = {0: (own[None], 0)}
    for name, sent, got, _ in STEPS:
        parts = [held[s][0][held[s][1]] for s in sent]
        if len(parts) > 1:
            parts = lax.optimization_barrier(parts)
        back = lax.ppermute(jnp.stack(parts), RING, plan.pairs[name])
        for i, s in enumerate(got):
            held[s] = (back, i)

    heads_in, state = (doc_lengths, q), None
    for j, call in enumerate(CALLS):
        state = attend(heads_in, call, [held[s] for s in call], state, j == len(CALLS) - 1)
        if j == 0:
            heads_in, state = state[:2], state[2:]
    out = lax.all_to_all(state, PLANE, split_axis=0, concat_axis=0, tiled=True)
    return unpack(out)


def solution(mesh):
    fine = Mesh(mesh.devices.reshape(4, 2, 4, 16, 2), AXES)
    spec = P(("y", "zl", "c"), ("x", "zh"), None)
    return jax.shard_map(
        functools.partial(body, Plan(4, 16, 2)),
        mesh=fine,
        in_specs=(spec, spec, spec, P()),
        out_specs=spec,
        check_vma=False,
    )
```

```python
import functools
import math

import jax
import jax.numpy as jnp
from jax import lax
from jax.experimental import pallas as pl
from jax.experimental.pallas import tpu as pltpu
from jax.sharding import Mesh
from jax.sharding import PartitionSpec as P


HD = 128
ROWS = 32
HEADS = 4
CHUNK = 64
NEG_FILL = -1e30
AXES = ("x", "zh", "y", "zl", "c")
PLANE = ("x", "c")
RING = ("zh", "y", "zl")

STEPS = (
    ("m1", (0,), (-9,), -9),
    ("p1", (0,), (3,), 3),
    ("p2", (3,), (6,), 3),
    ("e1", (0, 3), (1, 4), 1),
    ("m2", (-9,), (-12,), -3),
    ("e2", (6, -9), (7, -8), 1),
    ("m3", (-12,), (-15,), -3),
    ("g2", (1, 4, 7, -12), (2, 5, 8, -11), 1),
    ("g1", (-9, -12), (-10, -13), -1),
    ("h2", (-15,), (-14,), 1),
    ("h1", (-15,), (-16,), -1),
)
CALLS = (
    (0, 3),
    (6, 1, 4, -9),
    (7, -8, -12),
    (2, 5, 8, -10, -11, -13, -15),
    (-14, -16),
)


class Plan:
    def __init__(self, outer, half, halves):
        length, chips = half * halves, outer * half
        index = lambda z, y: ((z // half) * outer + y) * half + z % half
        where = {(z, y * half + z % half): index(z, y) for z in range(length) for y in range(outer)}
        held = {0: {key: key for key in where}}
        moves = {}
        for name, sent, got, shift in STEPS:
            target = {}
            for slot, new in zip(sent, got):
                held[new] = {}
                for (z, n), (zs, ns) in held[slot].items():
                    z2 = (z + shift) % length
                    to = (z2, (ns + (z2 - zs) % half) % chips)
                    assert target.setdefault((z, n), to) == to
                    held[new][to] = (zs, ns)
            assert len(set(target.values())) == len(target)
            moves[name] = target
        wanted = {s: {key for key in where if at[key][1] <= key[1]} for s, at in held.items()}
        self.pairs = {}
        for name, sent, got, shift in reversed(STEPS):
            used = {a: b for a, b in moves[name].items() if any(b in wanted[s] for s in got)}
            for slot, new in zip(sent, got):
                wanted[slot] |= {a for a, b in used.items() if b in wanted[new]}
            self.pairs[name] = [(where[a], where[b]) for a, b in sorted(used.items())]
        for (z, n) in where:
            want = {(h * half + m % half, m) for m in range(max(0, n - half // 2), n + 1) for h in range(halves)}
            got = [held[s][z, n] for call in CALLS for s in call]
            assert len(set(got)) == len(got) and want <= set(got)


def row_offsets(shape, dim):
    i = lax.broadcasted_iota(jnp.int32, shape, dim)
    return ((i >> 5) & 1) * 256 + (i >> 6) * 64 + (i & 31)


def document_bounds(lengths):
    count = lengths.shape[0]
    lane = lax.broadcasted_iota(jnp.int32, (1, HD), 1)
    begin = jnp.where(lane == count, -(1 << 24), 1 << 24)
    end = jnp.where(lane == count, 0, -(1 << 24))
    at = jnp.int32(0)
    for d in range(count):
        begin = jnp.where(lane == d, at, begin)
        at = at + lengths[d]
        end = jnp.where(lane == d, at, end)
    return begin, end


def attend_kernel(slots, first, last, *refs):
    count = len(slots)
    refs = list(refs)
    arrays = max(a for _, a, _ in slots) + 1
    if first:
        lengths, q_ref, *refs = refs
    else:
        bounds, q_all, top_in, acc_in, *refs = refs
    kv, refs = refs[:arrays], refs[arrays:]
    if last:
        out_ref, tops, *refs = refs
    elif first:
        bounds, q_all, tops, acc_out, *refs = refs
    else:
        tops, acc_out, *refs = refs
    k_all, v_all, *refs = refs
    scores, rounded = refs[:2], refs[2:]
    unit = math.log2(math.e) / math.sqrt(HD)
    half, halves = lax.axis_size("zl"), lax.axis_size("zh")

    chip = lax.axis_index("y") * half + lax.axis_index("zl")
    zh = lax.axis_index("zh")
    offsets = row_offsets((256, HD), 0)

    def members(base):
        return (offsets >= bounds[0:1] - base) & (offsets < bounds[1:2] - base)

    if first:
        begin, end = document_bounds(lengths)
        bounds[0:1], bounds[1:2] = begin, end
        apart = jnp.where(members(chip * 512 + zh * ROWS), 0.0, NEG_FILL).astype(jnp.bfloat16)
        for h in range(HEADS):
            q_all[h, :, :HD] = q_ref[:, h].reshape(256, HD)
            q_all[h, :, HD:] = apart

    def run():
        later = {}
        for j, (slot, a, i) in enumerate(slots):
            rows = slice(j * 256, (j + 1) * 256)
            back = slot if slot >= 0 else slot + half
            from_zh = ((zh * half + lax.axis_index("zl") - slot + half * halves) >> 4) & 1
            base = (chip - back) * 512 + from_zh * ROWS
            k_all[rows, :HD] = kv[a][i, :, 0].reshape(256, HD)
            k_all[rows, HD:] = jnp.where(members(base), 1.0, 0.0).astype(jnp.bfloat16)
            v_all[rows, :HD] = kv[a][i, :, 1].reshape(256, HD)
            if back == 0:
                later[j] = (from_zh - zh) * ROWS
        v_all[:, HD:] = jnp.ones((count * 256, HD), jnp.bfloat16)

        def score(h):
            scores[h & 1][...] = lax.dot_general(
                q_all[h], k_all[...], (((1,), (1,)), ((), ())), preferred_element_type=jnp.float32
            )

        def weigh(h):
            for r in range(0, 256, CHUNK):
                rows = slice(r, r + CHUNK)
                wide = None
                for j in range(count):
                    cols = slice(j * 256, (j + 1) * 256)
                    s = scores[h & 1][rows, cols]
                    if j in later:
                        q_at = row_offsets((256, 1), 0)[rows] - later[j]
                        s = jnp.where(row_offsets((1, 256), 1) <= q_at, s, NEG_FILL)
                        scores[h & 1][rows, cols] = s
                    wide = s if wide is None else jnp.maximum(wide, s)
                top = jnp.max(wide, axis=1, keepdims=True)
                if not first:
                    top = jnp.maximum(top_in[h, rows], top)
                for j in range(count):
                    cols = slice(j * 256, (j + 1) * 256)
                    w = jnp.exp2((scores[h & 1][rows, cols] - top) * unit)
                    rounded[h & 1][rows, cols] = w.astype(jnp.bfloat16)
                tops[h, rows] = top

        def gather(h):
            for r in range(0, 256, 128):
                rows = slice(r, r + 128)
                added = jnp.dot(rounded[h & 1][rows], v_all[...], preferred_element_type=jnp.float32)
                if not first:
                    factor = jnp.exp2((top_in[h, rows] - tops[h, rows]) * unit)
                    added = added + acc_in[h, rows] * factor
                if last:
                    res = added[:, :HD] / added[:, HD:]
                    out_ref[r // ROWS : r // ROWS + 4, h] = res.astype(jnp.bfloat16).reshape(4, ROWS, HD)
                else:
                    acc_out[h, rows] = added

        for h in range(HEADS + 2):
            if h < HEADS:
                score(h)
            if h >= 2:
                gather(h - 2)
            if 1 <= h <= HEADS:
                weigh(h - 1)

    nearest = min(s if s >= 0 else s + half for s, _, _ in slots)
    if first or last or nearest == 0:
        run()
        return
    pl.when(chip >= nearest)(run)

    @pl.when(chip < nearest)
    def _():
        tops[...] = top_in[...]
        acc_out[...] = acc_in[...]


VMEM = pl.BlockSpec(memory_space=pltpu.VMEM)
SMEM = pl.BlockSpec(memory_space=pltpu.SMEM)


def attend(heads_in, slots, blocks, state, last):
    n = len(blocks)
    first = state is None
    bounds = jax.ShapeDtypeStruct((8, HD), jnp.int32)
    q_all = jax.ShapeDtypeStruct((HEADS, 256, 2 * HD), jnp.bfloat16)
    top = jax.ShapeDtypeStruct((HEADS, 256, 1), jnp.float32)
    acc = jax.ShapeDtypeStruct((HEADS, 256, 2 * HD), jnp.float32)
    out = jax.ShapeDtypeStruct((8, HEADS, ROWS, HD), jnp.bfloat16)
    outs = out if last else (bounds, q_all, top, acc) if first else (top, acc)
    arrays = list({id(b): b for b, _ in blocks}.values())
    number = {id(b): a for a, b in enumerate(arrays)}
    where = tuple((s, number[id(b)], i) for s, (b, i) in zip(slots, blocks))
    return pl.pallas_call(
        functools.partial(attend_kernel, where, first, last),
        out_shape=outs,
        in_specs=([SMEM, VMEM] if first else [VMEM] * 4) + [VMEM] * len(arrays),
        out_specs=VMEM if last else tuple(VMEM for _ in outs),
        scratch_shapes=([pltpu.VMEM(top.shape, top.dtype)] if last else [])
        + [
            pltpu.VMEM((n * 256, 2 * HD), jnp.bfloat16),
            pltpu.VMEM((n * 256, 2 * HD), jnp.bfloat16),
            pltpu.VMEM((256, n * 256), jnp.float32),
            pltpu.VMEM((256, n * 256), jnp.float32),
            pltpu.VMEM((256, n * 256), jnp.bfloat16),
            pltpu.VMEM((256, n * 256), jnp.bfloat16),
        ],
        compiler_params=pltpu.CompilerParams(vmem_limit_bytes=(6 + 2 * n) << 20),
        cost_estimate=pl.CostEstimate(
            flops=n * HEADS * 256 * 256 * HD * 4,
            bytes_accessed=n * 131072 + 1500000,
            transcendentals=n * HEADS * 256 * 256,
        ),
    )(*heads_in, *(() if first else state), *arrays)


def copy_all(copies):
    for c in copies:
        c.start()
    for c in copies:
        c.wait()


def pack_kv_kernel(k_ref, v_ref, out_ref, sems):
    copy_all(
        [
            pltpu.make_async_copy(
                ref.at[0, :, g * HD : (g + 1) * HD], out_ref.at[g, part], sems.at[2 * g + part]
            )
            for g in range(8)
            for part, ref in enumerate((k_ref, v_ref))
        ]
    )


def pack_q_kernel(q_ref, out_ref, sems):
    copy_all(
        [
            pltpu.make_async_copy(
                q_ref.at[0, :, i * HD : (i + 1) * HD],
                out_ref.at[i // HEADS, i % HEADS],
                sems.at[i],
            )
            for i in range(8 * HEADS)
        ]
    )


def unpack_kernel(in_ref, out_ref, sems):
    copy_all(
        [
            pltpu.make_async_copy(
                in_ref.at[i // HEADS, i % HEADS],
                out_ref.at[0, :, i * HD : (i + 1) * HD],
                sems.at[i],
            )
            for i in range(8 * HEADS)
        ]
    )


def unpack(array):
    return pl.pallas_call(
        unpack_kernel,
        out_shape=jax.ShapeDtypeStruct((1, ROWS, 8 * HEADS * HD), jnp.bfloat16),
        in_specs=[VMEM],
        out_specs=pl.BlockSpec(memory_space=pltpu.HBM),
        scratch_shapes=[pltpu.SemaphoreType.DMA((8 * HEADS,))],
        compiler_params=pltpu.CompilerParams(vmem_limit_bytes=4 << 20),
    )(array)


def pack(kernel, shape, *arrays):
    return pl.pallas_call(
        kernel,
        out_shape=jax.ShapeDtypeStruct(shape, jnp.bfloat16),
        in_specs=[pl.BlockSpec(memory_space=pltpu.HBM)] * len(arrays),
        out_specs=VMEM,
        scratch_shapes=[pltpu.SemaphoreType.DMA((shape[0] * shape[1],))],
        compiler_params=pltpu.CompilerParams(vmem_limit_bytes=4 << 20),
    )(*[pltpu.with_memory_space_constraint(a, pltpu.HBM) for a in arrays])


def body(plan, *args):
    return spread(plan, *args)


def spread(plan, queries, keys, values, doc_lengths):
    kv = pack(pack_kv_kernel, (8, 2, ROWS, HD), keys, values)
    own = lax.all_to_all(kv, PLANE, split_axis=0, concat_axis=0, tiled=True)
    q = pack(pack_q_kernel, (8, HEADS, ROWS, HD), queries)
    q = lax.all_to_all(q, PLANE, split_axis=0, concat_axis=0, tiled=True)

    held = {0: (own[None], 0)}
    for name, sent, got, _ in STEPS:
        parts = [held[s][0][held[s][1]] for s in sent]
        if len(parts) > 1:
            parts = lax.optimization_barrier(parts)
        back = lax.ppermute(jnp.stack(parts), RING, plan.pairs[name])
        for i, s in enumerate(got):
            held[s] = (back, i)

    heads_in, state = (doc_lengths, q), None
    for j, call in enumerate(CALLS):
        state = attend(heads_in, call, [held[s] for s in call], state, j == len(CALLS) - 1)
        if j == 0:
            heads_in, state = state[:2], state[2:]
    out = lax.all_to_all(state, PLANE, split_axis=0, concat_axis=0, tiled=True)
    return unpack(out)


def solution(mesh):
    fine = Mesh(mesh.devices.reshape(4, 2, 4, 16, 2), AXES)
    spec = P(("y", "zl", "c"), ("x", "zh"), None)
    return jax.shard_map(
        functools.partial(body, Plan(4, 16, 2)),
        mesh=fine,
        in_specs=(spec, spec, spec, P()),
        out_specs=spec,
        check_vma=False,
    )
```
